32 devices in a mesh: dp: 4 (over x, core), tensor: 8 (over z, y).
Axes of the slice: x: 2, y: 2, z: 4, core: 2. Of those that a mesh axis runs over, the one named last changes fastest.
Arguments:
- out_grad: bfloat16 [2, 320, 4096], P(None, 'dp', 'tensor'), may hold values from -0.3125 to 0.3125
- layer_input: bfloat16 [2, 320, 4096], P(None, 'dp', 'tensor'), may hold values from -8 to 8
- w_down: bfloat16 [16384, 4096], P('tensor'), may hold values from -0.046875 to 0.046875
- silu_gate: bfloat16 [2, 320, 16384], P(None, 'dp', 'tensor'), may hold values from -6 to 6
- up_proj: bfloat16 [2, 320, 16384], P(None, 'dp', 'tensor'), may hold values from -6 to 6
- slope_codes: int32 [2, 32, 16384], P(None, 'dp', 'tensor'), may hold values from 0 to 1073741823
Outputs:
- grad_down: bfloat16 [16384, 4096], P('tensor', 'dp')
- grad_gate: bfloat16 [4096, 16384], P('dp', 'tensor')
- grad_up: bfloat16 [4096, 16384], P('dp', 'tensor')
The draws below stay inside these ranges and needn't reach their ends.
Inputs may be any that keep to these rules, and one draw needn't show every extreme that they name: `slope_codes`: every word holds ten independent 3-bit codes; all eight codes occur.
All inputs are finite; a program needn't handle non-finite values.
Results may differ from the reference program's by a relative error of at most 0.018.
Values may be sent and summed in bfloat16 or wider, within the bound.
A program may use at most 128 MiB of HBM per device.

```python
import jax
import jax.numpy as jnp
from jax import lax

D = 4096
FF = 16384
MICRO = 2
TOK_MB = 80
TOKENS = 320
N_DP = 4


def plant(values, key, smallest, top_value):
    longest = values.shape.index(max(values.shape))
    spots = []
    for shift in (0, 1):
        where = [jax.random.randint(jax.random.fold_in(key, axis), (), 0, length) for axis, length in enumerate(values.shape)]
        where[longest] = (where[longest] + shift) % values.shape[longest]
        spots.append(tuple(where))
    return values.at[spots[0]].set(smallest).at[spots[1]].set(top_value)


def spiked(drawn, stream_key, source, target, shards_of, factor):
    def block_of(axis_at):
        return (jnp.arange(drawn.shape[axis_at]) // (drawn.shape[axis_at] // shards_of)).reshape((-1,) + (1,) * (drawn.ndim - 1 - axis_at))

    near = jax.random.permutation(stream_key, shards_of)[block_of(target)]
    other_side = (block_of(target) + shards_of // 2) % shards_of
    return jnp.where((block_of(source) == near) | (block_of(source) == other_side), factor * drawn, drawn)


def levels(rng, extent, split, smallest, largest):
    gain = 1.0
    for axis_at, blocks in split:
        draws = jax.random.uniform(jax.random.fold_in(jax.random.fold_in(rng, 6), axis_at), (blocks,), jnp.float32, smallest / len(split), largest / len(split))
        gain = gain * jnp.repeat(jnp.exp(draws), extent[axis_at] // blocks).reshape((-1,) + (1,) * (len(extent) - 1 - axis_at))
    return gain


def normal_values(stream_key, shape, scale, limit, cuts=(), kind=jnp.bfloat16):
    level = levels(stream_key, shape, cuts, -0.22, 0.18) if cuts else 1.0
    array = jax.random.normal(stream_key, shape, jnp.float32) * scale * level
    return jnp.minimum(jnp.maximum(array, -limit), limit).astype(kind)


def heavy_noise(rng, shape, spread, reach, split, heavy, held_as=jnp.bfloat16):
    values = spread * jax.random.normal(rng, shape, jnp.float32)
    if split:
        values = values * levels(rng, shape, split, -0.22, 0.18)
    return jnp.clip(spiked(values, jax.random.fold_in(rng, 3), *heavy), -reach, reach).astype(held_as)


def setup_inputs(seed: int = 0) -> dict:
    streams_of = jax.random.split(jax.random.key(seed), 7)
    return {
        "out_grad": heavy_noise(streams_of[0], (MICRO, TOKENS, D), (1.0 / (MICRO * TOKENS) ** 0.5), 0.3125, ((1, 4), (2, 8)), (1, 2, 8, 2.0)),
        "layer_input": heavy_noise(streams_of[1], (MICRO, TOKENS, D), 1.0, 8.0, ((1, 4), (2, 8)), (1, 2, 8, 2.0)),
        "w_down": normal_values(streams_of[2], (FF, D), FF ** -0.5, 0.046875, ((0, 8),)),
        "silu_gate": normal_values(streams_of[3], (MICRO, TOKENS, FF), 1.0, 6.0, ((1, 4), (2, 8))),
        "up_proj": normal_values(streams_of[4], (MICRO, TOKENS, FF), 1.0, 6.0, ((1, 4), (2, 8))),
        "slope_codes": plant(jax.random.randint(streams_of[5], (MICRO, TOKENS // 10, FF), 0, 1073741824), jax.random.fold_in(streams_of[5], 1), 0, 1073741823).astype(jnp.int32),
    }


SLOPE_LEVELS = (-0.09, 0.06, 0.22, 0.41, 0.6, 0.79, 0.96, 1.08)


def decode_slopes(packed):
    shifts = 3 * jnp.arange(10, dtype=jnp.int32)
    pieces = jnp.bitwise_and(jnp.right_shift(packed[..., None, :], shifts[:, None]), 7)
    pieces = pieces.reshape(packed.shape[:-2] + (packed.shape[-2] * 10, packed.shape[-1]))
    result = jnp.full(pieces.shape, SLOPE_LEVELS[0], jnp.float32)
    for symbol in range(1, 8):
        result = jnp.where(pieces == symbol, jnp.float32(SLOPE_LEVELS[symbol]), result)
    return result


def rounded(values):
    return lax.optimization_barrier(values.astype(jnp.bfloat16)).astype(jnp.float32)


def by_group(values):
    columns = values.shape[-1]
    shaped = values.reshape(MICRO, N_DP, TOK_MB, columns).transpose(1, 0, 2, 3)
    return shaped.reshape(N_DP, MICRO * TOK_MB, columns)


def reference(out_grad, layer_input, w_down, silu_gate, up_proj, slope_codes):
    slopes = decode_slopes(slope_codes)
    hidden_grad = jnp.dot(out_grad.reshape(-1, D), w_down.T, preferred_element_type=jnp.float32)
    hidden_grad = hidden_grad.reshape(MICRO, -1, FF)
    gate_act = silu_gate.astype(jnp.float32)
    up_value = up_proj.astype(jnp.float32)
    up_grad = (hidden_grad * gate_act).astype(jnp.bfloat16)
    gate_grad = (hidden_grad * up_value * slopes).astype(jnp.bfloat16)
    hidden = (gate_act * up_value).astype(jnp.bfloat16)

    def add_group(totals, pieces):
        inputs, output_rows, hidden_rows, gate_rows, up_rows = pieces
        gate_part = jnp.dot(inputs.T, gate_rows, preferred_element_type=jnp.float32)
        up_part = jnp.dot(inputs.T, up_rows, preferred_element_type=jnp.float32)
        down_part = jnp.dot(hidden_rows.T, output_rows, preferred_element_type=jnp.float32)
        return (totals[0] + rounded(gate_part), totals[1] + rounded(up_part), totals[2] + rounded(down_part)), None

    start_totals = (jnp.zeros((D, FF), jnp.float32), jnp.zeros((D, FF), jnp.float32), jnp.zeros((FF, D), jnp.float32))
    totals, unused = lax.scan(add_group, start_totals, (by_group(layer_input), by_group(out_grad), by_group(hidden), by_group(gate_grad), by_group(up_grad)))
    return (totals[2].astype(jnp.bfloat16), totals[0].astype(jnp.bfloat16), totals[1].astype(jnp.bfloat16))
```

```python
import functools

import jax
import jax.numpy as jnp
from jax import lax
from jax.experimental import pallas as pl
from jax.experimental.pallas import tpu as pltpu
from jax.sharding import PartitionSpec as P

SLOPE_LEVELS = (-0.09, 0.06, 0.22, 0.41, 0.6, 0.79, 0.96, 1.08)
MESH = pl.DeviceIdType.MESH
CHUNKS = 4


def exchange(n_dp, n_t, out_ref, in_ref, silu_ref, up_ref, code_ref, spread_ref, w_ref,
             xg, hid_all, gate_all, up_all,
             og, wbuf, vbuf, own, stage,
             w_sem, p_send, p_recv, py_send, py_recv, og_sem,
             s_send, s_recv, h_send, h_sem, c_recv, zu_send, zd_send, y_send, y_recv,
             o_sem, o_send, o_recv, al_sem, ax_send, ax_recv, ac_send, ac_recv):
    chips = n_dp // 2
    rows = n_t // 2
    ratio = n_t // n_dp
    tokens, cols = out_ref.shape
    width = w_ref.shape[1]
    hidden = w_ref.shape[0]
    block = width // n_dp
    fc = hidden // CHUNKS
    units = 2 + 4 * (chips - 1)
    all_acts = (hid_all, gate_all, up_all)

    d = lax.axis_index("dp")
    t = lax.axis_index("tensor")
    q, c = d // 2, lax.rem(d, 2)
    z, y = t // 2, lax.rem(t, 2)
    partner = q * 2 + (1 - c)
    y_peer = z * 2 + (1 - y)
    owner = t // ratio
    owner_chip = owner // 2
    if ratio == 2:
        in_chain = d >= 0
        has_side = d >= 0
        chain_col, side_col = y, 1 - y
    else:
        in_chain = lax.rem(d, 2) == y
        has_side = lax.rem(d, 2) != y
        chain_col, side_col = y * 0, y * 0
    head_row = (d * ratio) // 2

    def chip_at(r):
        return lax.rem(q + r, chips) * 2 + c

    def row_at(k):
        return lax.rem(z + k, rows) * 2 + y

    def group_from(r, core):
        return lax.rem(q + chips - r, chips) * 2 + core

    def at_col(index, size):
        return pl.ds(pl.multiple_of(index * size, 128), size)

    def remote(src, dst, send, recv, dp, tensor):
        return pltpu.make_async_remote_copy(
            src_ref=src, dst_ref=dst, send_sem=send, recv_sem=recv,
            device_id={"dp": dp, "tensor": tensor}, device_id_type=MESH)

    barrier = pltpu.get_barrier_semaphore()
    greet = [(d, row_at(k)) for k in range(1, rows)] + [(d, y_peer), (partner, t)]
    greet += [(chip_at(r), t) for r in range(1, chips)]
    for dp, tensor in greet:
        pl.semaphore_signal(barrier, inc=1, device_id={"dp": dp, "tensor": tensor}, device_id_type=MESH)
    pl.semaphore_wait(barrier, len(greet))

    my_cols = og.at[:, at_col(t, cols)]

    def row_copy(k):
        return remote(out_ref, my_cols, p_send.at[k - 1], p_recv.at[k - 1], d, row_at(k))

    def row_wait(k):
        src = lax.rem(z + rows - k, rows) * 2 + y
        land = og.at[:, at_col(src, cols)]
        return remote(land, land, p_send.at[k - 1], p_recv.at[k - 1], d, y_peer)

    def side_copy(k):
        src = lax.rem(z + rows - k, rows) * 2 + y
        piece = og.at[:, at_col(src, cols)]
        return remote(out_ref if k == 0 else piece, piece, py_send.at[k], py_recv.at[k], d, y_peer)

    def side_wait(k):
        src = lax.rem(z + rows - k, rows) * 2 + (1 - y)
        piece = og.at[:, at_col(src, cols)]
        return remote(piece, piece, py_send.at[k], py_recv.at[k], d, y_peer)

    for k in range(1, rows):
        row_copy(k).start()
    side_copy(0).start()
    og_own = pltpu.make_async_copy(out_ref, my_cols, og_sem)
    og_own.start()

    away = owner_chip != q
    dist = lax.rem(owner_chip + chips - q, chips)
    slot = lax.max(dist - 1, 0)
    far = owner_chip * 2 + c

    def cross(a):
        src = in_ref if a == 0 else out_ref
        return remote(src, stage.at[a, slot], s_send.at[a], s_recv.at[a, slot], far, t)

    @pl.when(away)
    def _():
        for a in range(2):
            cross(a).start()

    def w_copy(j):
        part = pl.ds(pl.multiple_of(j * fc, 128), fc)
        return pltpu.make_async_copy(w_ref.at[part], wbuf.at[part], w_sem.at[j])

    for j in range(CHUNKS):
        w_copy(j).start()

    def unit_of(r, a):
        return 0 if r == 0 else 2 + (r - 1) * 4 + a * 2

    def hand(r, a, to_self):
        src = in_ref if r == 0 else stage.at[a, r - 1]
        u = unit_of(r, a) + c
        i = 0 if r == 0 else 1 + (r - 1) * 2 + a
        dst = xg.at[a, group_from(r, c), :, at_col(chain_col if ratio == 2 else 0, cols)]
        if to_self:
            return pltpu.make_async_copy(src, dst, c_recv.at[u])
        return remote(src, dst, h_send.at[i], c_recv.at[u], partner, t)

    source = owner_chip == q
    self_head = jnp.logical_and(source, owner == d)
    other_head = jnp.logical_and(source, owner != d)

    def hand_start(r, a):
        @pl.when(self_head)
        def _():
            hand(r, a, True).start()

        @pl.when(other_head)
        def _():
            hand(r, a, False).start()

    hand_start(0, 0)

    def f_part(j):
        return pl.ds(pl.multiple_of(j * fc, 128), fc)

    def own_local(a, j):
        return pltpu.make_async_copy(
            own.at[a, :, f_part(j)], all_acts[a].at[d, :, f_part(j)], al_sem.at[a, j])

    def own_chip(a, j, r):
        return remote(own.at[a, :, f_part(j)], all_acts[a].at[d, :, f_part(j)],
                      ax_send.at[a, r - 1, j], ax_recv.at[a, r - 1, j], chip_at(r), t)

    def own_core(a, j):
        return remote(own.at[a, :, f_part(j)], all_acts[a].at[d, :, f_part(j)],
                      ac_send.at[a, 0, j], ac_recv.at[a, 0, j], partner, t)

    def pass_core(a, j, r):
        land = all_acts[a].at[group_from(r, c), :, f_part(j)]
        return remote(land, land, ac_send.at[a, r, j], ac_recv.at[a, r, j], partner, t)

    def chip_wait(a, j, r):
        land = all_acts[a].at[group_from(r, c), :, f_part(j)]
        return remote(land, land, ax_send.at[a, r - 1, j], ax_recv.at[a, r - 1, j], partner, t)

    def core_wait(a, j, r):
        land = all_acts[a].at[group_from(r, 1 - c), :, f_part(j)]
        return remote(land, land, ac_send.at[a, r, j], ac_recv.at[a, r, j], partner, t)

    def send_own(a, j):
        for r in range(1, chips):
            own_chip(a, j, r).start()
        own_core(a, j).start()
        own_local(a, j).start()

    def early(j, carry):
        f = f_part(j)
        up_value = up_ref[:, f].astype(jnp.float32)
        own[0, :, f] = (silu_ref[:, f].astype(jnp.float32) * up_value).astype(jnp.bfloat16)
        words = code_ref[:, f]
        pieces = jnp.concatenate(
            [((words >> (3 * k)) & 7).astype(jnp.float32).astype(jnp.bfloat16) for k in range(10)], axis=0)
        symbols = jnp.dot(spread_ref[...], pieces, preferred_element_type=jnp.float32)
        slopes = jnp.full(symbols.shape, SLOPE_LEVELS[0], jnp.float32)
        for s in range(1, 8):
            slopes = jnp.where(symbols > s - 0.5, jnp.float32(SLOPE_LEVELS[s]), slopes)
        vbuf[:, f] = up_value * slopes
        send_own(0, j)
        return carry

    lax.fori_loop(0, CHUNKS, early, 0)

    for k in range(1, rows):
        row_wait(k).wait_recv()
        side_copy(k).start()

    for a in range(2):
        for r in range(1, chips):
            @pl.when(source)
            def _():
                land = stage.at[a, r - 1]
                remote(land, land, s_send.at[a], s_recv.at[a, r - 1], partner, t).wait_recv()
            hand_start(r, a)

    og_own.wait()
    for k in range(rows):
        side_wait(k).wait_recv()

    o_own = pltpu.make_async_copy(og.at[:, at_col(d, block)], xg.at[1, d], o_sem)
    o_own.start()
    o_other = remote(og.at[:, at_col(partner, block)], xg.at[1, d], o_send, o_recv, partner, t)
    o_other.start()

    go_up = jnp.logical_and(in_chain, jnp.logical_and(z >= head_row, z + 1 < rows))
    go_down = jnp.logical_and(in_chain, jnp.logical_and(z <= head_row, z > 0))
    z_up = lax.min(z + 1, rows - 1) * 2 + y
    z_down = lax.max(z - 1, 0) * 2 + y

    def unit_ref(u, col):
        v = lax.max(u - 2, 0)
        far_unit = u >= 2
        r = jnp.where(far_unit, v // 4 + 1, 0)
        a = jnp.where(far_unit, lax.rem(v // 2, 2), 0)
        core = lax.rem(u, 2)
        return xg.at[a, group_from(r, core), :, at_col(col, cols)]

    def chain(u):
        piece = unit_ref(u, chain_col)
        return (remote(piece, piece, zu_send.at[u], c_recv.at[u], d, z_up),
                remote(piece, piece, zd_send.at[u], c_recv.at[u], d, z_down),
                remote(piece, piece, y_send.at[u], y_recv.at[u], d, y_peer))

    def chain_step(u):
        up_copy, down_copy, across = chain(u)

        @pl.when(in_chain)
        def _():
            up_copy.wait_recv()

        @pl.when(go_up)
        def _():
            up_copy.start()

        @pl.when(go_down)
        def _():
            down_copy.start()

        @pl.when(in_chain)
        def _():
            across.start()

    per = -(-units // CHUNKS)

    def late(j, carry):
        f = f_part(j)
        w_copy(j).wait()
        grad = lax.dot_general(og[...], wbuf[f, :], (((1,), (1,)), ((), ())),
                               preferred_element_type=jnp.float32)
        own[1, :, f] = (grad * vbuf[:, f]).astype(jnp.bfloat16)
        own[2, :, f] = (grad * silu_ref[:, f].astype(jnp.float32)).astype(jnp.bfloat16)
        send_own(1, j)
        send_own(2, j)
        for i in range(per):
            u = j * per + i

            @pl.when(u < units)
            def _():
                chain_step(u)
        return carry

    lax.fori_loop(0, CHUNKS, late, 0)

    def relay(a):
        def step(j, carry):
            for r in range(1, chips):
                chip_wait(a, j, r).wait_recv()
                pass_core(a, j, r).start()
            return carry
        return step

    lax.fori_loop(0, CHUNKS, relay(0), 0)

    def relay_late(j, carry):
        relay(1)(j, carry)
        return relay(2)(j, carry)

    lax.fori_loop(0, CHUNKS, relay_late, 0)

    for k in range(1, rows):
        row_copy(k).wait_send()
    for k in range(rows):
        side_copy(k).wait_send()

    @pl.when(away)
    def _():
        for a in range(2):
            cross(a).wait_send()

    @pl.when(other_head)
    def _():
        for r in range(chips):
            for a in range(2):
                if r or not a:
                    hand(r, a, False).wait_send()

    o_own.wait()
    o_other.wait()

    def unit_end(u, carry):
        up_copy, down_copy, across = chain(u)

        @pl.when(go_up)
        def _():
            up_copy.wait_send()

        @pl.when(go_down)
        def _():
            down_copy.wait_send()

        @pl.when(in_chain)
        def _():
            across.wait_send()

        @pl.when(has_side)
        def _():
            piece = unit_ref(u, side_col)
            remote(piece, piece, y_send.at[u], y_recv.at[u], d, y_peer).wait_recv()
        return carry

    lax.fori_loop(0, units, unit_end, 0)

    def act_end(j, carry):
        for a in range(3):
            own_local(a, j).wait()
            own_core(a, j).wait_send()
            core_wait(a, j, 0).wait_recv()
            for r in range(1, chips):
                own_chip(a, j, r).wait_send()
                pass_core(a, j, r).wait_send()
                core_wait(a, j, r).wait_recv()
        return carry

    lax.fori_loop(0, CHUNKS, act_end, 0)


def shards(n_dp, n_t, out_grad, layer_input, w_down, silu_gate, up_proj, slope_codes):
    hidden, width = w_down.shape
    cols = out_grad.shape[2]
    tokens = out_grad.shape[0] * out_grad.shape[1]
    chips, rows, block = n_dp // 2, n_t // 2, width // n_dp
    words = tokens // 10
    row = lax.broadcasted_iota(jnp.int32, (tokens, tokens), 0)
    col = lax.broadcasted_iota(jnp.int32, (tokens, tokens), 1)
    spread = (col == (row % 10) * words + row // 10).astype(jnp.bfloat16)
    units = 2 + 4 * (chips - 1)
    far = chips - 1
    bf16 = jnp.bfloat16
    dma = pltpu.SemaphoreType.DMA
    vmem = pl.BlockSpec(memory_space=pltpu.VMEM)
    anywhere = pl.BlockSpec(memory_space=pl.ANY)
    acts = jax.ShapeDtypeStruct((n_dp, tokens, hidden), bf16)
    flops = 2 * tokens * hidden * width
    xg, hid, gate, up = pl.pallas_call(
        functools.partial(exchange, n_dp, n_t),
        out_shape=(jax.ShapeDtypeStruct((2, n_dp, tokens, block), bf16), acts, acts, acts),
        in_specs=[vmem] * 6 + [anywhere],
        out_specs=[anywhere] * 4,
        scratch_shapes=[
            pltpu.VMEM((tokens, width), bf16),
            pltpu.VMEM((hidden, width), bf16),
            pltpu.VMEM((tokens, hidden), jnp.float32),
            pltpu.VMEM((3, tokens, hidden), bf16),
            pltpu.VMEM((2, far, tokens, cols), bf16),
            dma((CHUNKS,)),
            dma((rows - 1,)), dma((rows - 1,)), dma((rows,)), dma((rows,)), dma,
            dma((2,)), dma((2, far)), dma((1 + 2 * far,)), dma,
            dma((units,)), dma((units,)), dma((units,)), dma((units,)), dma((units,)),
            dma, dma, dma,
            dma((3, CHUNKS)), dma((3, far, CHUNKS)), dma((3, far, CHUNKS)),
            dma((3, chips, CHUNKS)), dma((3, chips, CHUNKS)),
        ],
        compiler_params=pltpu.CompilerParams(
            collective_id=0, has_side_effects=True, vmem_limit_bytes=60 * 1024 * 1024),
        cost_estimate=pl.CostEstimate(flops=flops, bytes_accessed=50_000_000, transcendentals=0),
    )(
        out_grad.reshape(tokens, cols), layer_input.reshape(tokens, cols),
        silu_gate.reshape(tokens, hidden), up_proj.reshape(tokens, hidden),
        slope_codes.reshape(words, hidden), spread, w_down,
    )
    total = n_dp * tokens
    inputs, outputs = xg[0].reshape(total, block), xg[1].reshape(total, block)
    over_rows = (((0,), (0,)), ((), ()))

    def product(left, right):
        return lax.dot_general(left, right, over_rows, preferred_element_type=jnp.float32).astype(bf16)

    return (
        product(hid.reshape(total, hidden), outputs),
        product(inputs, gate.reshape(total, hidden)),
        product(inputs, up.reshape(total, hidden)),
    )


def solution(mesh):
    n_dp, n_t = mesh.shape["dp"], mesh.shape["tensor"]
    return jax.shard_map(
        functools.partial(shards, n_dp, n_t),
        mesh=mesh,
        in_specs=(
            P(None, "dp", "tensor"),
            P(None, "dp", "tensor"),
            P("tensor", None),
            P(None, "dp", "tensor"),
            P(None, "dp", "tensor"),
            P(None, "dp", "tensor"),
        ),
        out_specs=(P("tensor", "dp"), P("dp", "tensor"), P("dp", "tensor")),
        check_vma=False,
    )
```

```python
import functools

import jax
import jax.numpy as jnp
import numpy as np
from jax import lax
from jax.experimental import pallas as pl
from jax.experimental.pallas import tpu as pltpu
from jax.sharding import PartitionSpec as P

SLOPE_LEVELS = (-0.09, 0.06, 0.22, 0.41, 0.6, 0.79, 0.96, 1.08)
MESH = pl.DeviceIdType.MESH
CHUNKS = 4


def exchange(n_dp, n_t, out_ref, in_ref, silu_ref, up_ref, code_ref, spread_ref, w_ref,
             xin, xout, hid_all, gate_all, up_all,
             og, wbuf, vbuf, own, stage,
             w_sem, p_send, p_recv, py_send, py_recv, og_sem,
             s_send, s_recv, h_send, h_sem, c_recv, zu_send, zd_send, y_send, y_recv,
             o_sem, o_send, o_recv, al_sem, ax_send, ax_recv, ac_send, ac_recv):
    chips = n_dp // 2
    rows = n_t // 2
    ratio = n_t // n_dp
    tokens, cols = out_ref.shape
    width = w_ref.shape[1]
    hidden = w_ref.shape[0]
    block = width // n_dp
    fc = hidden // CHUNKS
    units = 2 + 4 * (chips - 1)
    xg = (xin, xout)
    all_acts = (hid_all, gate_all, up_all)

    d = lax.axis_index("dp")
    t = lax.axis_index("tensor")
    q, c = d // 2, lax.rem(d, 2)
    z, y = t // 2, lax.rem(t, 2)
    partner = q * 2 + (1 - c)
    y_peer = z * 2 + (1 - y)
    owner = t // ratio
    owner_chip = owner // 2
    if ratio == 2:
        in_chain = d >= 0
        has_side = d >= 0
        chain_col, side_col = y, 1 - y
    else:
        in_chain = lax.rem(d, 2) == y
        has_side = lax.rem(d, 2) != y
        chain_col, side_col = y * 0, y * 0
    head_row = (d * ratio) // 2

    def chip_at(r):
        return lax.rem(q + r, chips) * 2 + c

    def row_at(k):
        return lax.rem(z + k, rows) * 2 + y

    def group_from(r, core):
        return lax.rem(q + chips - r, chips) * 2 + core

    def at_col(index, size):
        return pl.ds(pl.multiple_of(index * size, 128), size)

    def remote(src, dst, send, recv, dp, tensor):
        return pltpu.make_async_remote_copy(
            src_ref=src, dst_ref=dst, send_sem=send, recv_sem=recv,
            device_id={"dp": dp, "tensor": tensor}, device_id_type=MESH)

    barrier = pltpu.get_barrier_semaphore()
    greet = [(d, row_at(k)) for k in range(1, rows)] + [(d, y_peer), (partner, t)]
    greet += [(chip_at(r), t) for r in range(1, chips)]
    for dp, tensor in greet:
        pl.semaphore_signal(barrier, inc=1, device_id={"dp": dp, "tensor": tensor}, device_id_type=MESH)
    pl.semaphore_wait(barrier, len(greet))

    my_cols = og.at[:, at_col(t, cols)]

    def row_copy(k):
        return remote(out_ref, my_cols, p_send.at[k - 1], p_recv.at[k - 1], d, row_at(k))

    def row_wait(k):
        src = lax.rem(z + rows - k, rows) * 2 + y
        land = og.at[:, at_col(src, cols)]
        return remote(land, land, p_send.at[k - 1], p_recv.at[k - 1], d, y_peer)

    def side_copy(k):
        src = lax.rem(z + rows - k, rows) * 2 + y
        piece = og.at[:, at_col(src, cols)]
        return remote(out_ref if k == 0 else piece, piece, py_send.at[k], py_recv.at[k], d, y_peer)

    def side_wait(k):
        src = lax.rem(z + rows - k, rows) * 2 + (1 - y)
        piece = og.at[:, at_col(src, cols)]
        return remote(piece, piece, py_send.at[k], py_recv.at[k], d, y_peer)

    for k in range(1, rows):
        row_copy(k).start()
    side_copy(0).start()
    og_own = pltpu.make_async_copy(out_ref, my_cols, og_sem)
    og_own.start()

    away = owner_chip != q
    dist = lax.rem(owner_chip + chips - q, chips)
    slot = lax.max(dist - 1, 0)
    far = owner_chip * 2 + c

    def cross(a):
        src = in_ref if a == 0 else out_ref
        return remote(src, stage.at[a, slot], s_send.at[a], s_recv.at[a, slot], far, t)

    @pl.when(away)
    def _():
        for a in range(2):
            cross(a).start()

    def w_copy(j):
        part = pl.ds(pl.multiple_of(j * fc, 128), fc)
        return pltpu.make_async_copy(w_ref.at[part], wbuf.at[part], w_sem.at[j])

    for j in range(CHUNKS):
        w_copy(j).start()

    def unit_of(r, a):
        return 0 if r == 0 else 2 + (r - 1) * 4 + a * 2

    def hand(r, a, to_self):
        src = in_ref if r == 0 else stage.at[a, r - 1]
        u = unit_of(r, a) + c
        i = 0 if r == 0 else 1 + (r - 1) * 2 + a
        dst = xg[a].at[group_from(r, c), :, at_col(chain_col if ratio == 2 else 0, cols)]
        if to_self:
            return pltpu.make_async_copy(src, dst, c_recv.at[u])
        return remote(src, dst, h_send.at[i], c_recv.at[u], partner, t)

    source = owner_chip == q
    self_head = jnp.logical_and(source, owner == d)
    other_head = jnp.logical_and(source, owner != d)

    def hand_start(r, a):
        @pl.when(self_head)
        def _():
            hand(r, a, True).start()

        @pl.when(other_head)
        def _():
            hand(r, a, False).start()

    hand_start(0, 0)

    def f_part(j):
        return pl.ds(pl.multiple_of(j * fc, 128), fc)

    def own_local(a, j):
        return pltpu.make_async_copy(
            own.at[a, :, f_part(j)], all_acts[a].at[d, :, f_part(j)], al_sem.at[a, j])

    def own_chip(a, j, r):
        return remote(own.at[a, :, f_part(j)], all_acts[a].at[d, :, f_part(j)],
                      ax_send.at[a, r - 1, j], ax_recv.at[a, r - 1, j], chip_at(r), t)

    def own_core(a, j):
        return remote(own.at[a, :, f_part(j)], all_acts[a].at[d, :, f_part(j)],
                      ac_send.at[a, 0, j], ac_recv.at[a, 0, j], partner, t)

    def pass_core(a, j, r):
        land = all_acts[a].at[group_from(r, c), :, f_part(j)]
        return remote(land, land, ac_send.at[a, r, j], ac_recv.at[a, r, j], partner, t)

    def chip_wait(a, j, r):
        land = all_acts[a].at[group_from(r, c), :, f_part(j)]
        return remote(land, land, ax_send.at[a, r - 1, j], ax_recv.at[a, r - 1, j], partner, t)

    def core_wait(a, j, r):
        land = all_acts[a].at[group_from(r, 1 - c), :, f_part(j)]
        return remote(land, land, ac_send.at[a, r, j], ac_recv.at[a, r, j], partner, t)

    def send_own(a, j):
        for r in range(1, chips):
            own_chip(a, j, r).start()
        own_core(a, j).start()
        own_local(a, j).start()

    def early(j, carry):
        f = f_part(j)
        up_value = up_ref[:, f].astype(jnp.float32)
        own[0, :, f] = (silu_ref[:, f].astype(jnp.float32) * up_value).astype(jnp.bfloat16)
        words = code_ref[:, f]
        pieces = jnp.concatenate(
            [((words >> (3 * k)) & 7).astype(jnp.float32).astype(jnp.bfloat16) for k in range(10)], axis=0)
        symbols = jnp.dot(spread_ref[...], pieces, preferred_element_type=jnp.float32)
        slopes = jnp.full(symbols.shape, SLOPE_LEVELS[0], jnp.float32)
        for s in range(1, 8):
            slopes = jnp.where(symbols > s - 0.5, jnp.float32(SLOPE_LEVELS[s]), slopes)
        vbuf[:, f] = up_value * slopes
        send_own(0, j)
        return carry

    lax.fori_loop(0, CHUNKS, early, 0)

    for k in range(1, rows):
        row_wait(k).wait_recv()
        side_copy(k).start()

    for a in range(2):
        for r in range(1, chips):
            @pl.when(source)
            def _():
                land = stage.at[a, r - 1]
                remote(land, land, s_send.at[a], s_recv.at[a, r - 1], partner, t).wait_recv()
            hand_start(r, a)

    go_up = jnp.logical_and(in_chain, jnp.logical_and(z >= head_row, z + 1 < rows))
    go_down = jnp.logical_and(in_chain, jnp.logical_and(z <= head_row, z > 0))
    z_up = lax.min(z + 1, rows - 1) * 2 + y
    z_down = lax.max(z - 1, 0) * 2 + y

    def unit_ref(u, col):
        r, a, core = (0, 0, u) if u < 2 else ((u - 2) // 4 + 1, (u - 2) // 2 % 2, u % 2)
        return xg[a].at[group_from(r, core), :, at_col(col, cols)]

    def chain(u):
        piece = unit_ref(u, chain_col)
        return (remote(piece, piece, zu_send.at[u], c_recv.at[u], d, z_up),
                remote(piece, piece, zd_send.at[u], c_recv.at[u], d, z_down),
                remote(piece, piece, y_send.at[u], y_recv.at[u], d, y_peer))

    at_head = jnp.logical_and(in_chain, z == head_row)
    past_head = jnp.logical_and(in_chain, z != head_row)

    def chain_step(u, role):
        up_copy, down_copy, across = chain(u)

        @pl.when(role)
        def _():
            up_copy.wait_recv()

        @pl.when(jnp.logical_and(role, go_up))
        def _():
            up_copy.start()

        @pl.when(jnp.logical_and(role, go_down))
        def _():
            down_copy.start()

        @pl.when(role)
        def _():
            across.start()

    per = -(-units // CHUNKS)

    for u in range(units):
        chain_step(u, at_head)

    og_own.wait()
    for k in range(rows):
        side_wait(k).wait_recv()

    o_own = pltpu.make_async_copy(og.at[:, at_col(d, block)], xg[1].at[d], o_sem)
    o_own.start()
    o_other = remote(og.at[:, at_col(partner, block)], xg[1].at[d], o_send, o_recv, partner, t)
    o_other.start()

    def late(j, carry):
        f = f_part(j)
        w_copy(j).wait()
        grad = lax.dot_general(og[...], wbuf[f, :], (((1,), (1,)), ((), ())),
                               preferred_element_type=jnp.float32)
        own[1, :, f] = (grad * vbuf[:, f]).astype(jnp.bfloat16)
        own[2, :, f] = (grad * silu_ref[:, f].astype(jnp.float32)).astype(jnp.bfloat16)
        send_own(1, j)
        send_own(2, j)
        return carry

    lax.fori_loop(0, CHUNKS, late, 0)

    def relay(a):
        def step(j, carry):
            for r in range(1, chips):
                chip_wait(a, j, r).wait_recv()
                pass_core(a, j, r).start()
            return carry
        return step

    lax.fori_loop(0, CHUNKS, relay(0), 0)

    def relay_late(j, carry):
        relay(1)(j, carry)
        return relay(2)(j, carry)

    for j in range(CHUNKS):
        for u in range(j * per, min((j + 1) * per, units)):
            chain_step(u, past_head)
        relay_late(j, 0)

    for k in range(1, rows):
        row_copy(k).wait_send()
    for k in range(rows):
        side_copy(k).wait_send()

    @pl.when(away)
    def _():
        for a in range(2):
            cross(a).wait_send()

    @pl.when(other_head)
    def _():
        for r in range(chips):
            for a in range(2):
                if r or not a:
                    hand(r, a, False).wait_send()

    o_own.wait()
    o_other.wait()

    def unit_end(u):
        up_copy, down_copy, across = chain(u)

        @pl.when(go_up)
        def _():
            up_copy.wait_send()

        @pl.when(go_down)
        def _():
            down_copy.wait_send()

        @pl.when(in_chain)
        def _():
            across.wait_send()

        @pl.when(has_side)
        def _():
            piece = unit_ref(u, side_col)
            remote(piece, piece, y_send.at[u], y_recv.at[u], d, y_peer).wait_recv()

    for u in range(units):
        unit_end(u)

    def act_end(j, carry):
        for a in range(3):
            own_local(a, j).wait()
            own_core(a, j).wait_send()
            core_wait(a, j, 0).wait_recv()
            for r in range(1, chips):
                own_chip(a, j, r).wait_send()
                pass_core(a, j, r).wait_send()
                core_wait(a, j, r).wait_recv()
        return carry

    lax.fori_loop(0, CHUNKS, act_end, 0)


def products(in_ref, out_ref, hid_ref, gate_ref, up_ref, down_grad, gate_grad, up_grad, turned):
    @pl.when(pl.program_id(0) == 0)
    def _():
        turned[...] = in_ref[...].T

    def product(left, right):
        return jnp.dot(left, right, preferred_element_type=jnp.float32).astype(jnp.bfloat16)

    gate_grad[...] = product(turned[...], gate_ref[...])
    up_grad[...] = product(turned[...], up_ref[...])
    down_grad[...] = product(hid_ref[...].T, out_ref[...])


def shards(n_dp, n_t, out_grad, layer_input, w_down, silu_gate, up_proj, slope_codes):
    hidden, width = w_down.shape
    cols = out_grad.shape[2]
    tokens = out_grad.shape[0] * out_grad.shape[1]
    chips, rows, block = n_dp // 2, n_t // 2, width // n_dp
    words = tokens // 10
    row, col = np.arange(tokens)[:, None], np.arange(tokens)[None, :]
    spread = jnp.asarray(col == (row % 10) * words + row // 10, jnp.bfloat16)
    units = 2 + 4 * (chips - 1)
    far = chips - 1
    bf16 = jnp.bfloat16
    dma = pltpu.SemaphoreType.DMA
    vmem = pl.BlockSpec(memory_space=pltpu.VMEM)
    anywhere = pl.BlockSpec(memory_space=pl.ANY)
    acts = jax.ShapeDtypeStruct((n_dp, tokens, hidden), bf16)
    rows_of_block = jax.ShapeDtypeStruct((n_dp, tokens, block), bf16)
    flops = 2 * tokens * hidden * width
    xin, xout, hid, gate, up = pl.pallas_call(
        functools.partial(exchange, n_dp, n_t),
        out_shape=(rows_of_block, rows_of_block, acts, acts, acts),
        in_specs=[vmem] * 6 + [anywhere],
        out_specs=[anywhere] * 5,
        scratch_shapes=[
            pltpu.VMEM((tokens, width), bf16),
            pltpu.VMEM((hidden, width), bf16),
            pltpu.VMEM((tokens, hidden), jnp.float32),
            pltpu.VMEM((3, tokens, hidden), bf16),
            pltpu.VMEM((2, far, tokens, cols), bf16),
            dma((CHUNKS,)),
            dma((rows - 1,)), dma((rows - 1,)), dma((rows,)), dma((rows,)), dma,
            dma((2,)), dma((2, far)), dma((1 + 2 * far,)), dma,
            dma((units,)), dma((units,)), dma((units,)), dma((units,)), dma((units,)),
            dma, dma, dma,
            dma((3, CHUNKS)), dma((3, far, CHUNKS)), dma((3, far, CHUNKS)),
            dma((3, chips, CHUNKS)), dma((3, chips, CHUNKS)),
        ],
        compiler_params=pltpu.CompilerParams(
            collective_id=0, has_side_effects=True, vmem_limit_bytes=60 * 1024 * 1024),
        cost_estimate=pl.CostEstimate(flops=flops, bytes_accessed=50_000_000, transcendentals=0),
    )(
        out_grad.reshape(tokens, cols), layer_input.reshape(tokens, cols),
        silu_gate.reshape(tokens, hidden), up_proj.reshape(tokens, hidden),
        slope_codes.reshape(words, hidden), spread, w_down,
    )
    total = n_dp * tokens
    inputs, outputs = xin.reshape(total, block), xout.reshape(total, block)
    piece = min(512, hidden)
    whole = pl.BlockSpec((total, block), lambda i: (0, 0))
    part = pl.BlockSpec((total, piece), lambda i: (0, i))
    tall = pl.BlockSpec((block, piece), lambda i: (0, i))
    across = jax.ShapeDtypeStruct((block, hidden), bf16)
    return pl.pallas_call(
        products,
        grid=(hidden // piece,),
        out_shape=(jax.ShapeDtypeStruct((hidden, block), bf16), across, across),
        in_specs=[whole, whole, part, part, part],
        out_specs=[pl.BlockSpec((piece, block), lambda i: (i, 0)), tall, tall],
        scratch_shapes=[pltpu.VMEM((block, total), bf16)],
        compiler_params=pltpu.CompilerParams(vmem_limit_bytes=60 * 1024 * 1024),
    )(
        inputs, outputs, hid.reshape(total, hidden),
        gate.reshape(total, hidden), up.reshape(total, hidden),
    )


def solution(mesh):
    n_dp, n_t = mesh.shape["dp"], mesh.shape["tensor"]
    return jax.shard_map(
        functools.partial(shards, n_dp, n_t),
        mesh=mesh,
        in_specs=(
            P(None, "dp", "tensor"),
            P(None, "dp", "tensor"),
            P("tensor", None),
            P(None, "dp", "tensor"),
            P(None, "dp", "tensor"),
            P(None, "dp", "tensor"),
        ),
        out_specs=(P("tensor", "dp"), P("dp", "tensor"), P("dp", "tensor")),
        check_vma=False,
    )
```
